32 devices in a mesh: genes: 16 (over z, y, core), cols: 2 (over x).
Axes of the slice: x: 2, y: 2, z: 4, core: 2. Of those that a mesh axis runs over, the one named last changes fastest.
Arguments:
- expression: float32 [384, 40960], P(None, ('genes', 'cols')), may hold values from -200 to 200
- resample: int32 [384], replicated, may hold values from 0 to 383
- labels: int32 [40960, 300], P(('genes', 'cols')), may hold values from 0 to 1, as said below
- ref_kim: float32 [40960], P(('genes', 'cols')), may hold values from 0 to 1
Outputs:
- connectivity: float32 [40960, 300], P(('genes', 'cols'))
- preservation: float32 [2, 300], replicated
The draws below stay inside these ranges and needn't reach their ends.
Inputs may be any that keep to these rules, and one draw needn't show every extreme that they name: `labels`: each row holds exactly one 1; every module has 32 or more genes.
All inputs are finite; a program needn't handle non-finite values.
Results may differ from the reference program's by a relative error of at most 0.0031.
Values may be sent and summed in bfloat16 or wider, within the bound.
A program may use at most 128 MiB of HBM per device.

```python
import math
import jax
import jax.numpy as jnp
from jax import lax

G = 40960
K = 300
SAMPLES = 384
MIN_MODULE = 32


def gene_modules(key):
    order = jax.random.permutation(jax.random.fold_in(key, 11), G)
    position = jnp.arange(G, dtype=jnp.int32)
    extra = jax.random.randint(jax.random.fold_in(key, 12), (G,), 0, K, dtype=jnp.int32)
    at_position = jnp.where(position < K * MIN_MODULE, position % K, extra)
    return jnp.zeros((G,), jnp.int32).at[order].set(at_position)


def draw_labels(key, part):
    module_ids = gene_modules(key)
    return (module_ids[:, None] == jnp.arange(K, dtype=jnp.int32)[None, :]).astype(jnp.int32)


def shared_signal(key, module_ids):
    meta_count = 8
    meta = jnp.clip(jax.random.normal(jax.random.fold_in(key, 26), (SAMPLES, meta_count), jnp.float32), -6.0, 6.0)
    mixing = jax.random.uniform(jax.random.fold_in(key, 27), (meta_count, K), jnp.float32, 0.3, 1.0)
    mixing = mixing / jnp.sqrt(jnp.sum(mixing * mixing, axis=0, keepdims=True))
    shares = jax.random.uniform(jax.random.fold_in(key, 28), (K,), jnp.float32, 0.4, 0.8)
    own = jnp.clip(jax.random.normal(jax.random.fold_in(key, 21), (SAMPLES, K), jnp.float32), -6.0, 6.0)
    common = jnp.dot(meta, mixing, precision=lax.Precision.HIGHEST, preferred_element_type=jnp.float32)
    factor = jnp.clip(jnp.sqrt(shares)[None, :] * common + jnp.sqrt(1.0 - shares)[None, :] * own, -6.0, 6.0)
    loading = jax.random.uniform(jax.random.fold_in(key, 22), (G,), jnp.float32, 0.5, 2.0)
    gene_mix = jax.random.normal(jax.random.fold_in(key, 29), (meta_count, G), jnp.float32) / jnp.sqrt(jnp.float32(meta_count))
    direct = jnp.clip(0.4 * jnp.dot(meta, gene_mix, precision=lax.Precision.HIGHEST, preferred_element_type=jnp.float32), -3.0, 3.0)
    return jnp.take(factor, module_ids, axis=1) * loading[None, :] + direct


def draw_expression(key, part):
    module_ids = gene_modules(key)
    signal = shared_signal(key, module_ids)
    noise = jnp.clip(jax.random.normal(jax.random.fold_in(key, 23), (SAMPLES, G), jnp.float32), -6.0, 6.0)
    return signal + noise


def place_ends(array, key, least, top_value):
    shape = array.shape
    spot = [jax.random.randint(jax.random.fold_in(key, axis), (), 0, shape[axis]) for axis in range(len(shape))]
    array = array.at[tuple(spot)].set(least)
    longest = shape.index(max(shape))
    spot[longest] = (spot[longest] + 1) % shape[longest]
    return array.at[tuple(spot)].set(top_value)


def level_of(own_key, shape, split, least, high):
    level = 1.0
    for dim, shards_of in split:
        draws = jax.random.uniform(jax.random.fold_in(jax.random.fold_in(own_key, 6), dim), (shards_of,), jnp.float32, least / len(split), high / len(split))
        level = level * jnp.repeat(jnp.exp(draws), shape[dim] // shards_of).reshape((-1,) + (1,) * (len(shape) - 1 - dim))
    return level


def setup_inputs(seed: int = 0) -> dict:
    key_of = jax.random.split(jax.random.key(seed), 5)
    return {
        "expression": draw_expression(jax.random.fold_in(key_of[4], 71), 0),
        "resample": place_ends(jax.random.randint(key_of[1], (SAMPLES,), 0, SAMPLES), jax.random.fold_in(key_of[1], 1), 0, SAMPLES - 1).astype(jnp.int32),
        "labels": draw_labels(jax.random.fold_in(key_of[4], 71), 0),
        "ref_kim": jnp.clip(1.0 * jax.random.uniform(key_of[3], (G,), jnp.float32) ** level_of(key_of[3], (G,), ((0, 32),), -0.2, 0.2), 0.0, 1.0),
    }


def standardize(expression, resample):
    boot = jnp.take(expression, resample, axis=0)
    centered = boot - lax.optimization_barrier(jnp.mean(boot, axis=0, keepdims=True))
    total = lax.optimization_barrier(jnp.sum(centered * centered, axis=0, keepdims=True))
    return (centered * lax.rsqrt(total + 1e-06)).astype(jnp.bfloat16)

def local_sums(connectivity, labels, ref_kim):
    member = labels.astype(jnp.float32)
    kim = lax.optimization_barrier(jnp.sum(connectivity * member, axis=1))
    rowsum = lax.optimization_barrier(jnp.sum(connectivity, axis=1))
    stacked = jnp.stack([kim, kim * kim, ref_kim, ref_kim * ref_kim, kim * ref_kim, rowsum, jnp.ones_like(kim)], axis=1)
    return jnp.dot(member.T, stacked, precision=lax.Precision.HIGHEST, preferred_element_type=jnp.float32)

def preserve(sums, total_genes):
    counts = sums[:, 6]
    mean_x = sums[:, 0] / (counts * counts)
    var_x = jnp.maximum(sums[:, 1] / (counts * counts * counts) - mean_x * mean_x, 0.0001)
    mean_y = sums[:, 2] / counts
    var_y = jnp.maximum(sums[:, 3] / counts - mean_y * mean_y, 0.01)
    cross = sums[:, 4] / (counts * counts) - mean_x * mean_y
    between = (sums[:, 5] - sums[:, 0]) / (counts * (total_genes - counts))
    density = (mean_x - between) * jnp.sqrt(counts / var_x)
    linked = cross * jnp.sqrt(counts / (var_x * var_y))
    return jnp.stack([density, linked], axis=0)

def reference(expression, resample, labels, ref_kim):
    scaled = standardize(expression, resample)
    member_bf = labels.astype(jnp.bfloat16)
    block_rows = math.gcd(G, 512)

    def one_block(block_index):
        rows = lax.dynamic_slice_in_dim(scaled, block_index * block_rows, block_rows, 1)
        scores = lax.dot_general(rows, scaled, (((0,), (0,)), ((), ())), preferred_element_type=jnp.float32)
        squares = scores * scores
        adjacency = (squares * squares * squares).astype(jnp.bfloat16)
        return jnp.dot(adjacency, member_bf, preferred_element_type=jnp.float32)
    pieces = lax.map(one_block, jnp.arange(G // block_rows, dtype=jnp.int32))
    connectivity = pieces.reshape(G, K)
    sums = local_sums(connectivity, labels, ref_kim)
    return (connectivity, preserve(sums, G))
```

```python
import functools

import jax
import jax.numpy as jnp
from jax import lax
from jax.experimental import pallas as pl
from jax.experimental.pallas import tpu as pltpu
from jax.sharding import PartitionSpec as P

G = 40960
MESH = pl.DeviceIdType.MESH
ID_LANES = 256
ID_BASE = 16
TILE = 256


def round_up(value, unit):
    return -(-value // unit) * unit


def ring_chip(position, chips):
    half = chips // 2
    return jnp.where(position < half, 2 * position, 2 * (chips - 1 - position) + 1)


def ring_position(chip, chips):
    level = chip // 2
    return jnp.where(lax.rem(chip, 2) == 0, level, chips - 1 - level)


def network_kernel(
    chips, width, block_hbm, rows_hbm, out_ref,
    slots, rows, member, powers, total, outgoing, incoming,
    local_sem, ring_send, ring_recv, pair_send, pair_recv, row_sem, half_sem,
):
    genes_at = lax.axis_index("genes")
    cols_at = lax.axis_index("cols")
    core = lax.rem(genes_at, 2)
    chip = genes_at // 2
    position = ring_position(chip, chips)
    after = lax.rem(position + 1, chips)
    before = lax.rem(position + chips - 1, chips)
    forward = jnp.where(core == 0, after, before)
    backward = jnp.where(core == 0, before, after)
    next_device = (ring_chip(forward, chips) * 2 + core, cols_at)
    last_device = (ring_chip(backward, chips) * 2 + core, cols_at)
    pair_device = (chip * 2 + 1 - core, cols_at)
    side_device = (genes_at, 1 - cols_at)

    load_block = pltpu.make_async_copy(block_hbm, slots.at[0], local_sem.at[0])
    load_rows = pltpu.make_async_copy(rows_hbm, rows.at[0], local_sem.at[1])
    load_block.start()
    load_rows.start()
    barrier = pltpu.get_barrier_semaphore()
    for device in (next_device, last_device, pair_device, side_device):
        pl.semaphore_signal(barrier, inc=1, device_id=device, device_id_type=MESH)
    total[...] = jnp.zeros_like(total)
    load_block.wait()
    load_rows.wait()
    pl.semaphore_wait(barrier, 4)

    def ring_copy(step):
        return pltpu.make_async_remote_copy(
            src_ref=slots.at[2 * step], dst_ref=slots.at[2 * step + 2],
            send_sem=ring_send.at[step], recv_sem=ring_recv.at[step],
            device_id=next_device, device_id_type=MESH,
        )

    def pair_copy(step):
        return pltpu.make_async_remote_copy(
            src_ref=slots.at[2 * step], dst_ref=slots.at[2 * step + 1],
            send_sem=pair_send.at[step], recv_sem=pair_recv.at[step],
            device_id=pair_device, device_id_type=MESH,
        )

    row_copy = pltpu.make_async_remote_copy(
        src_ref=rows.at[0], dst_ref=rows.at[1],
        send_sem=row_sem.at[0], recv_sem=row_sem.at[1],
        device_id=side_device, device_id_type=MESH,
    )

    modules = member.shape[0]
    id_rows = -(-width // ID_LANES)
    tile = TILE if width % TILE == 0 else width

    def set_members(slot):
        coded = slots[slot, width:, :ID_LANES].astype(jnp.float32)
        names = lax.broadcasted_iota(jnp.int32, (modules, ID_LANES), 0).astype(jnp.float32)
        for row in range(id_rows):
            ids = coded[row : row + 1] * ID_BASE + coded[id_rows + row : id_rows + row + 1]
            lanes = min(ID_LANES, width - row * ID_LANES)
            hit = jnp.where(names == ids, 1.0, 0.0).astype(jnp.bfloat16)
            member[:, row * ID_LANES : row * ID_LANES + lanes] = hit[:, :lanes]

    def add_block(slot, halves):
        set_members(slot)

        def one_tile(index, carry):
            spot = pl.ds(pl.multiple_of(index * tile, tile), tile)
            for half in halves:
                scores = lax.dot_general(
                    slots[slot, :width, :], rows[half, spot, :], (((1,), (1,)), ((), ())),
                    preferred_element_type=jnp.float32,
                )
                squares = scores * scores
                powers[half] = (squares * squares * squares).astype(jnp.bfloat16)
            for half in halves:
                total[half, :, spot] += jnp.dot(
                    member[:, :width], powers[half], preferred_element_type=jnp.float32
                )
            return carry

        lax.fori_loop(0, width // tile, one_tile, 0)

    ring_copy(0).start()
    pair_copy(0).start()
    row_copy.start()
    add_block(0, (0,))
    pair_copy(0).wait_recv()
    add_block(1, (0,))
    row_copy.wait_recv()

    def early(slot, carry):
        add_block(slot, (1,))
        return carry

    lax.fori_loop(0, 2, early, 0)

    def one_step(step, carry):
        ring_copy(step - 1).wait_recv()
        ring_copy(step).start()
        pair_copy(step).start()
        add_block(2 * step, (0, 1))
        pair_copy(step).wait_recv()
        add_block(2 * step + 1, (0, 1))
        return carry

    lax.fori_loop(1, chips - 1, one_step, 0)

    end = chips - 1
    ring_copy(end - 1).wait_recv()
    pair_copy(end).start()
    add_block(2 * end, (1,))
    pair_copy(end).wait_recv()
    add_block(2 * end + 1, (1,))
    outgoing[...] = total[1, :, :width].astype(jnp.bfloat16)
    half_copy = pltpu.make_async_remote_copy(
        src_ref=outgoing, dst_ref=incoming,
        send_sem=half_sem.at[0], recv_sem=half_sem.at[1],
        device_id=side_device, device_id_type=MESH,
    )
    half_copy.start()

    def late(index, carry):
        add_block(2 * end + index, (0,))
        return carry

    lax.fori_loop(0, 2, late, 0)

    def drain(step, carry):
        ring_copy(step).wait_send()
        pair_copy(step).wait_send()
        return carry

    lax.fori_loop(0, end, drain, 0)
    pair_copy(end).wait_send()
    row_copy.wait_send()
    half_copy.wait()
    out_ref[...] = total[0, :, :width] + incoming[...].astype(jnp.float32)


def network(block, rows, chips, module_rows, collective_id):
    width, depth = rows.shape
    padded = round_up(width, 128)
    dma = pltpu.SemaphoreType.DMA
    return pl.pallas_call(
        functools.partial(network_kernel, chips, width),
        out_shape=jax.ShapeDtypeStruct((module_rows, width), jnp.float32),
        in_specs=[pl.BlockSpec(memory_space=pl.ANY)] * 2,
        out_specs=pl.BlockSpec(memory_space=pltpu.VMEM),
        scratch_shapes=[
            pltpu.VMEM((2 * chips, block.shape[0], depth), jnp.bfloat16),
            pltpu.VMEM((2, width, depth), jnp.bfloat16),
            pltpu.VMEM((module_rows, padded), jnp.bfloat16),
            pltpu.VMEM((2, width, TILE if width % TILE == 0 else width), jnp.bfloat16),
            pltpu.VMEM((2, module_rows, padded), jnp.float32),
            pltpu.VMEM((module_rows, width), jnp.bfloat16),
            pltpu.VMEM((module_rows, width), jnp.bfloat16),
            dma((2,)), dma((chips,)), dma((chips,)), dma((chips,)), dma((chips,)),
            dma((2,)), dma((2,)),
        ],
        compiler_params=pltpu.CompilerParams(
            collective_id=collective_id, has_side_effects=True, vmem_limit_bytes=60 * 1024 * 1024
        ),
    )(block, rows)


def total_kernel(stages, value_ref, out_ref, parts, send_sem, recv_sem):
    genes_at = lax.axis_index("genes")
    cols_at = lax.axis_index("cols")

    def peer(stage, offset):
        axis, stride, count = stage
        if axis == "cols":
            return (genes_at, lax.rem(cols_at + offset, count))
        digit = lax.rem(genes_at // stride, count)
        return (genes_at + (lax.rem(digit + offset, count) - digit) * stride, cols_at)

    barrier = pltpu.get_barrier_semaphore()
    peers = 0
    for stage in stages:
        for offset in range(1, stage[2]):
            pl.semaphore_signal(barrier, inc=1, device_id=peer(stage, offset), device_id_type=MESH)
            peers += 1
    pl.semaphore_wait(barrier, peers)
    base = 0
    current = value_ref[...]
    for stage in stages:
        parts[base] = current
        copies = []
        for offset in range(1, stage[2]):
            copies.append(pltpu.make_async_remote_copy(
                src_ref=parts.at[base], dst_ref=parts.at[base + offset],
                send_sem=send_sem.at[base + offset], recv_sem=recv_sem.at[base + offset],
                device_id=peer(stage, offset), device_id_type=MESH,
            ))
            copies[-1].start()
        for copy in copies:
            copy.wait()
        digit = cols_at if stage[0] == "cols" else lax.rem(genes_at // stage[1], stage[2])
        count = stage[2]
        current = parts[base + lax.rem(digit, count)]
        for origin in range(1, count):
            current = current + parts[base + lax.rem(digit - origin + count, count)]
        base += count
    out_ref[...] = current


def total_sum(value, stages, collective_id):
    slots = sum(stage[2] for stage in stages)
    return pl.pallas_call(
        functools.partial(total_kernel, stages),
        out_shape=jax.ShapeDtypeStruct(value.shape, value.dtype),
        in_specs=[pl.BlockSpec(memory_space=pltpu.VMEM)],
        out_specs=pl.BlockSpec(memory_space=pltpu.VMEM),
        scratch_shapes=[
            pltpu.VMEM((slots,) + value.shape, value.dtype),
            pltpu.SemaphoreType.DMA((slots,)),
            pltpu.SemaphoreType.DMA((slots,)),
        ],
        compiler_params=pltpu.CompilerParams(collective_id=collective_id, has_side_effects=True),
    )(value)


def preserve(sums, total_genes):
    counts = sums[6]
    mean_x = sums[0] / (counts * counts)
    var_x = jnp.maximum(sums[1] / (counts * counts * counts) - mean_x * mean_x, 0.0001)
    mean_y = sums[2] / counts
    var_y = jnp.maximum(sums[3] / counts - mean_y * mean_y, 0.01)
    cross = sums[4] / (counts * counts) - mean_x * mean_y
    between = (sums[5] - sums[0]) / (counts * (total_genes - counts))
    density = (mean_x - between) * jnp.sqrt(counts / var_x)
    linked = cross * jnp.sqrt(counts / (var_x * var_y))
    return jnp.stack([density, linked], axis=0)


def local(genes_size, cols_size, expression, resample, labels, ref_kim):
    samples, width = expression.shape
    module_count = labels.shape[1]
    module_rows = round_up(module_count, 16)
    chips = genes_size // 2
    sample_ids = jnp.arange(samples, dtype=jnp.int32)
    counts = jnp.sum(
        (resample[:, None] == sample_ids[None, :]).astype(jnp.float32), axis=0
    )
    weights = counts[:, None]
    mean = jnp.sum(expression * weights, axis=0, keepdims=True) / resample.shape[0]
    centered = expression - mean
    spread = jnp.sum(centered * centered * weights, axis=0, keepdims=True)
    scaled = (centered * lax.rsqrt(spread + 1e-06)).astype(jnp.bfloat16)
    module_ids = jnp.sum(labels * jnp.arange(module_count, dtype=jnp.int32)[None, :], axis=1)

    id_rows = -(-width // ID_LANES)
    coded = jnp.pad(module_ids, (0, id_rows * ID_LANES - width)).reshape(id_rows, ID_LANES)
    coded = jnp.concatenate([coded // ID_BASE, lax.rem(coded, ID_BASE)], axis=0)
    block_rows = round_up(width + 2 * id_rows, 16)
    coded = jnp.pad(
        coded.astype(jnp.bfloat16), ((0, block_rows - width - 2 * id_rows), (0, 0))
    )
    drawn = counts > 0
    place = jnp.cumsum(drawn.astype(jnp.int32)) - 1

    def at_depth(depth, collective_id):
        def run(_):
            kept = (place[None, :] == jnp.arange(depth, dtype=jnp.int32)[:, None]) & drawn[None, :]
            kept_bf = kept.astype(jnp.bfloat16)
            packed = lax.dot_general(
                scaled, kept_bf, (((0,), (1,)), ((), ())), preferred_element_type=jnp.float32
            )
            kept_counts = jnp.sum(jnp.where(kept, counts[None, :], 0.0), axis=1)
            rows = (packed * kept_counts[None, :]).astype(jnp.bfloat16)
            tail = jnp.pad(coded, ((0, 0), (0, depth - ID_LANES)))
            block = jnp.concatenate([packed.astype(jnp.bfloat16), tail], axis=0)
            return network(block, rows, chips, module_rows, collective_id)

        return run

    short = 256
    distinct = jnp.sum(drawn.astype(jnp.int32))
    if samples > short:
        by_module = lax.cond(
            distinct <= short, at_depth(short, 1), at_depth(round_up(samples, 128), 2), 0
        )
    else:
        by_module = at_depth(short, 1)(0)

    by_module = by_module[:module_count]
    connectivity = by_module.T
    member = (
        jnp.arange(module_count, dtype=jnp.int32)[:, None] == module_ids[None, :]
    ).astype(jnp.float32)
    kim = jnp.sum(by_module * member, axis=0)
    rowsum = jnp.sum(by_module, axis=0)
    stacked = jnp.stack(
        [kim, kim * kim, ref_kim, ref_kim * ref_kim, kim * ref_kim, rowsum,
         jnp.ones_like(kim), jnp.zeros_like(kim)],
        axis=0,
    )
    sums = lax.dot_general(
        stacked, member, (((1,), (1,)), ((), ())),
        precision=lax.Precision.HIGHEST, preferred_element_type=jnp.float32,
    )
    sums = jnp.pad(sums, ((0, 0), (0, round_up(module_count, 128) - module_count)))
    stages = (("genes", 1, 2), ("cols", 1, cols_size), ("genes", 2, 2), ("genes", 4, genes_size // 4))
    sums = total_sum(sums, stages, 3)[:, :module_count]
    return (connectivity, preserve(sums, G))


def solution(mesh):
    placed = (P(None, ("genes", "cols")), P(), P(("genes", "cols"), None), P(("genes", "cols")))
    return jax.shard_map(
        functools.partial(local, mesh.shape["genes"], mesh.shape["cols"]),
        mesh=mesh,
        in_specs=placed,
        out_specs=(P(("genes", "cols"), None), P()),
        check_vma=False,
    )
```
